32 devices in a mesh: dp: 8 (over z, y), owner: 4 (over x, core).
Axes of the slice: x: 2, y: 2, z: 4, core: 2. Of those that a mesh axis runs over, the one named last changes fastest.
Arguments:
- gradients: bfloat16 [8, 4, 512, 512], P('dp', 'owner'), may hold values from -600 to 600
- block_layer: int32 [4], P('owner'), may hold values from 0 to 3
Outputs:
- update: bfloat16 [4, 512, 512], P('owner', 'dp')
The draws below stay inside these ranges and needn't reach their ends.
All inputs are finite; a program needn't handle non-finite values.
Results may differ from the reference program's by a relative error of at most 0.0062.
Values may be sent and summed in bfloat16 or wider, within the bound.
A program may use at most 64 MiB of HBM per device.

```python
import math
import jax
import jax.numpy as jnp
from jax import lax

B = 512
LAYERS = 4
ITERS = 3
NBLK = 4
N_DP = 8


def draw_gradients(key, part):
    first_key = jax.random.fold_in(jax.random.fold_in(key, 11), 0)
    third_key = jax.random.fold_in(jax.random.fold_in(key, 11), 2)
    fourth_key = jax.random.fold_in(jax.random.fold_in(key, 11), 3)
    fifth_key = jax.random.fold_in(jax.random.fold_in(key, 11), 4)
    scales = jnp.exp(jax.random.uniform(first_key, (N_DP, NBLK, 1, 1), jnp.float32, 0.0, math.log(10.0)))
    heavy = jax.random.randint(fourth_key, (1, NBLK, 1, 1), 0, N_DP)
    replica_ids = jnp.arange(N_DP, dtype=jnp.int32)[:, None, None, None]
    scales = jnp.where(replica_ids == heavy, 25.0, scales)
    row_place = jnp.arange(B, dtype=jnp.float32)[None, None, :, None] / float(B - 1)
    jitter = jnp.exp(jax.random.uniform(fifth_key, (1, NBLK, B, 1), jnp.float32, math.log(0.8), math.log(1.25)))
    ramp = jnp.exp(0.5 * math.log(10.0) * row_place) * jitter
    values = jnp.clip(jax.random.normal(third_key, (N_DP, NBLK, B, B), jnp.float32), -6.0, 6.0)
    return (scales * ramp * values).astype(jnp.bfloat16)


def with_ends(array, stream_key, low, high):
    extent = array.shape
    place = [jax.random.randint(jax.random.fold_in(stream_key, axis), (), 0, extent[axis]) for axis in range(len(extent))]
    array = array.at[tuple(place)].set(low)
    longest = extent.index(max(extent))
    place[longest] = (place[longest] + 1) % extent[longest]
    return array.at[tuple(place)].set(high)


def setup_inputs(seed: int = 0) -> dict:
    arg_keys = jax.random.split(jax.random.key(seed), 3)
    return {
        "gradients": draw_gradients(jax.random.fold_in(arg_keys[2], 71), 0),
        "block_layer": with_ends(jax.random.randint(arg_keys[1], (NBLK,), 0, LAYERS), jax.random.fold_in(arg_keys[1], 1), 0, LAYERS - 1).astype(jnp.int32),
    }


def inverse_root(statistic):
    size_b = statistic.shape[0]
    identity = jnp.eye(size_b, dtype=jnp.float32)
    ridge_term = 0.01 * jnp.trace(statistic) / size_b + 1e-06
    shifted = statistic + ridge_term * identity
    scaling = jnp.sqrt(jnp.sum(shifted * shifted))
    current = shifted / scaling
    inverse = identity
    for step_number in range(ITERS):
        factor = (5.0 * identity - current) / 4.0
        if step_number == 0:
            inverse = scaling ** (-0.25) * factor
        else:
            inverse = jnp.dot(inverse, factor, precision=lax.Precision.HIGHEST)
        if step_number + 1 < ITERS:
            square = jnp.dot(factor, factor, precision=lax.Precision.HIGHEST)
            fourth = jnp.dot(square, square, precision=lax.Precision.HIGHEST)
            current = jnp.dot(fourth, current, precision=lax.Precision.HIGHEST)
    return inverse

def one_block(block_grads):
    widened = block_grads.astype(jnp.float32)
    left_sum = jnp.einsum('dij,dkj->ik', widened, widened, precision=lax.Precision.HIGHEST)
    right_sum = jnp.einsum('dji,djk->ik', widened, widened, precision=lax.Precision.HIGHEST)
    left_root = lax.optimization_barrier(inverse_root(left_sum).astype(jnp.bfloat16)).astype(jnp.float32)
    right_root = lax.optimization_barrier(inverse_root(right_sum).astype(jnp.bfloat16)).astype(jnp.float32)
    total_sum = lax.optimization_barrier(jnp.sum(widened, axis=0))
    middle = jnp.dot(left_root, total_sum, precision=lax.Precision.HIGHEST)
    return jnp.dot(middle, right_root, precision=lax.Precision.HIGHEST) / N_DP

def reference(gradients, block_layer):
    precond = lax.map(one_block, jnp.swapaxes(gradients, 0, 1))
    energy = lax.optimization_barrier(jnp.sum(precond * precond, axis=(1, 2)))
    selector = (block_layer[:, None] == jnp.arange(LAYERS, dtype=jnp.int32)[None, :]).astype(jnp.float32)
    layer_energy = lax.optimization_barrier(jnp.sum(selector * energy[:, None], axis=0))
    layer_count = lax.optimization_barrier(jnp.sum(selector, axis=0)) * float(B * B)
    block_mean = lax.optimization_barrier(jnp.sum(selector * layer_energy[None, :], axis=1)) / lax.optimization_barrier(jnp.sum(selector * layer_count[None, :], axis=1))
    return (precond * lax.rsqrt(block_mean + 1e-06)[:, None, None]).astype(jnp.bfloat16)
```

```python
import functools

import jax
import jax.numpy as jnp
from jax import lax
from jax.experimental import pallas as pl
from jax.experimental.pallas import tpu as pltpu
from jax.sharding import PartitionSpec as P

LAYERS = 4
ITERS = 3
TILE = 128
BF16 = jnp.bfloat16
F32 = jnp.float32
MESH = pl.DeviceIdType.MESH


def mm(a, b):
    return jnp.dot(a.astype(BF16), b.astype(BF16), preferred_element_type=F32)


def upper_tiles(size_b):
    t = size_b // TILE
    return [(i, j) for i in range(t) for j in range(i, t)]


def pack(gram, acc_ref, size_b):
    tiles = upper_tiles(size_b)
    for n, (i, j) in enumerate(tiles):
        block = gram[i * TILE:(i + 1) * TILE, j * TILE:(j + 1) * TILE]
        acc_ref[n * TILE:(n + 1) * TILE, :] = block.astype(BF16)
    used, rows = len(tiles) * TILE, acc_ref.shape[0]
    if rows > used:
        acc_ref[used:, :] = jnp.zeros((rows - used, TILE), BF16)


def unpack(gath_ref, stat_ref, size_b):
    for n, (i, j) in enumerate(upper_tiles(size_b)):
        block = gath_ref[n * TILE:(n + 1) * TILE, :].astype(F32)
        stat_ref[i * TILE:(i + 1) * TILE, j * TILE:(j + 1) * TILE] = block
        if i != j:
            stat_ref[j * TILE:(j + 1) * TILE, i * TILE:(i + 1) * TILE] = block.T


def inverse_root(stat_ref, size_b):
    rows = lax.broadcasted_iota(jnp.int32, (size_b, size_b), 0)
    cols = lax.broadcasted_iota(jnp.int32, (size_b, size_b), 1)
    diag = rows == cols
    stat = stat_ref[...]
    trace = jnp.sum(jnp.where(diag, stat, 0.0), keepdims=True)
    ridge = 0.01 * trace / size_b + 1e-06
    shifted = stat + jnp.where(diag, ridge, 0.0)
    norm2 = jnp.sum(shifted * shifted, keepdims=True)
    m = shifted * lax.rsqrt(norm2)
    a, y = 1.25, -0.25 * m
    for step in range(1, ITERS):
        square = mm(m, m)
        once = (25.0 * m - 10.0 * square + mm(m, square)) * 0.0625
        m = 1.5625 * once + mm((square - 10.0 * m) * 0.0625, once)
        y = 1.25 * y - (0.25 * a) * m - 0.25 * mm(y, m)
        a = 1.25 * a
    scale = lax.rsqrt(jnp.sqrt(jnp.sqrt(norm2)))
    return scale * (y + jnp.where(diag, a, 0.0))


class Piece:
    def __init__(self, index, me, order, acc, gath, landing, send, recv, target):
        self.index, self.me, self.order = index, me, order
        self.acc, self.gath, self.landing = acc, gath, landing
        self.send, self.recv, self.target = send, recv, target
        self.start_row, self.length = 0, acc.shape[0]
        self.copy, self.offset = None, 0

    def bit(self, number):
        d = 1 << number
        mine = self.me // d % 2
        return mine, self.me + d * (1 - 2 * mine)

    def rows(self, first, length):
        return pl.ds(pl.multiple_of(first, 16), length)

    def start(self, step):
        nb = len(self.order)
        if step < nb:
            mine, partner = self.bit(self.order[step])
            half = self.length // 2
            src = self.acc.at[self.rows(self.start_row + (1 - mine) * half, half)]
            dst = self.landing.at[pl.ds(self.offset, half)]
        else:
            mine, partner = self.bit(self.order[2 * nb - 1 - step])
            here = self.rows(self.start_row, self.length)
            src, dst = self.gath.at[here], self.gath.at[here]
        self.copy = pltpu.make_async_remote_copy(
            src_ref=src,
            dst_ref=dst,
            send_sem=self.send.at[self.index, step],
            recv_sem=self.recv.at[self.index, step],
            device_id=self.target(partner),
            device_id_type=MESH,
        )
        self.copy.start()

    def finish(self, step):
        nb = len(self.order)
        self.copy.wait()
        if step < nb:
            mine, _ = self.bit(self.order[step])
            half = self.length // 2
            first = self.start_row + mine * half
            keep = self.rows(first, half)
            arrived = self.landing[pl.ds(self.offset, half), :].astype(F32)
            total = (self.acc[keep, :].astype(F32) + arrived).astype(BF16)
            (self.acc if step + 1 < nb else self.gath)[keep, :] = total
            self.start_row, self.length = first, half
            self.offset += half
        else:
            mine, _ = self.bit(self.order[2 * nb - 1 - step])
            self.start_row = self.start_row - mine * self.length
            self.length *= 2


def kernel(dp_count, owners, layer_ref, g_ref, out_ref, acc_s, gath_s, land_s, acc_g, gath_g,
           land_g, stats, roots, precond, e_src, e_buf, send, recv, e_send, e_recv):
    me = lax.axis_index("dp")
    own = lax.axis_index("owner")
    size_b = g_ref.shape[0]
    nb = dp_count.bit_length() - 1

    barrier = pltpu.get_barrier_semaphore()
    for number in range(nb):
        d = 1 << number
        partner = me + d * (1 - 2 * (me // d % 2))
        pl.semaphore_signal(barrier, inc=1, device_id=(partner, own), device_id_type=MESH)
    for j in range(1, owners):
        pl.semaphore_signal(
            barrier, inc=1, device_id=(me, lax.rem(own + j, owners)), device_id_type=MESH
        )

    order_a = list(range(nb))
    order_b = order_a[1::-1] + order_a[2:]
    target = lambda partner: (partner, own)
    stat_pieces = [
        Piece(i, me, order, acc_s.at[i], gath_s.at[i], land_s.at[i], send, recv, target)
        for i, order in enumerate((order_a, order_b))
    ]
    grad_pieces = [
        Piece(2 + i, me, order, acc_g.at[i], gath_g.at[i], land_g.at[i], send, recv, target)
        for i, order in enumerate((order_a, order_b))
    ]
    g = g_ref[...]
    width = size_b // 2
    left = lax.dot_general(g, g, (((1,), (1,)), ((), ())), preferred_element_type=F32)
    pack(left, acc_s.at[0], size_b)
    pl.semaphore_wait(barrier, nb + owners - 1)
    stat_pieces[0].start(0)
    right = lax.dot_general(g, g, (((0,), (0,)), ((), ())), preferred_element_type=F32)
    pack(right, acc_s.at[1], size_b)
    stat_pieces[1].start(0)
    for i in range(2):
        acc_g[i] = g[:, i * width:(i + 1) * width]
        grad_pieces[i].start(0)

    steps = 2 * nb
    for step in range(steps):
        for piece in stat_pieces:
            piece.finish(step)
            if step + 1 < steps:
                piece.start(step + 1)
        if step + 1 < steps:
            for piece in grad_pieces:
                piece.finish(step)
                piece.start(step + 1)

    def solve(i, carry):
        unpack(gath_s.at[i], stats, size_b)
        roots[i] = inverse_root(stats, size_b).astype(BF16)
        return carry

    lax.fori_loop(0, 2, solve, 0)
    for piece in grad_pieces:
        piece.finish(steps - 1)

    for i in range(2):
        cols = slice(i * width, (i + 1) * width)
        stats[:, cols] = jnp.dot(roots[0], gath_g[i], preferred_element_type=F32)
    middle = stats[...]
    high = middle.astype(BF16)
    low = (middle - high.astype(F32)).astype(BF16)
    right_root = roots[1]
    whole = jnp.dot(high, right_root, preferred_element_type=F32)
    whole += jnp.dot(low, right_root, preferred_element_type=F32)
    whole = whole / dp_count
    precond[...] = whole
    energy = jnp.sum(whole * whole, keepdims=True)

    layer = layer_ref[0]
    sub = lax.broadcasted_iota(jnp.int32, e_src.shape, 0)
    lane = lax.broadcasted_iota(jnp.int32, e_src.shape, 1)
    mine = lane == layer
    value = jnp.where(sub == 0, energy, float(size_b * size_b))
    e_src[...] = jnp.where(mine, value, 0.0)
    copies = []
    for j in range(1, owners):
        copy = pltpu.make_async_remote_copy(
            src_ref=e_src,
            dst_ref=e_buf.at[j - 1],
            send_sem=e_send.at[j - 1],
            recv_sem=e_recv.at[j - 1],
            device_id=(me, lax.rem(own + j, owners)),
            device_id_type=MESH,
        )
        copy.start()
        copies.append(copy)
    totals = e_src[...]
    for j, copy in enumerate(copies):
        copy.wait()
        totals += e_buf[j]
    energies = jnp.sum(jnp.where(mine & (sub == 0), totals, 0.0), keepdims=True)
    counts = jnp.sum(jnp.where(mine & (sub == 1), totals, 0.0), keepdims=True)
    height = out_ref.shape[0]
    rows = precond[pl.ds(pl.multiple_of(me * height, 16), height), :]
    out_ref[...] = (rows * lax.rsqrt(energies / counts + 1e-06)).astype(BF16)


def per_device(dp_count, owners, gradients, block_layer):
    size_b = gradients.shape[-1]
    nb = dp_count.bit_length() - 1
    used = len(upper_tiles(size_b)) * TILE
    unit = 16 * dp_count
    packed = -(-used // unit) * unit
    height = size_b // dp_count
    width = size_b // 2
    out = pl.pallas_call(
        functools.partial(kernel, dp_count, owners),
        out_shape=jax.ShapeDtypeStruct((height, size_b), BF16),
        in_specs=[
            pl.BlockSpec(memory_space=pltpu.SMEM),
            pl.BlockSpec(memory_space=pltpu.VMEM),
        ],
        out_specs=pl.BlockSpec(memory_space=pltpu.VMEM),
        scratch_shapes=[
            pltpu.VMEM((2, packed, TILE), BF16),
            pltpu.VMEM((2, packed, TILE), BF16),
            pltpu.VMEM((2, packed, TILE), BF16),
            pltpu.VMEM((2, size_b, width), BF16),
            pltpu.VMEM((2, size_b, width), BF16),
            pltpu.VMEM((2, size_b, width), BF16),
            pltpu.VMEM((size_b, size_b), F32),
            pltpu.VMEM((2, size_b, size_b), BF16),
            pltpu.VMEM((size_b, size_b), F32),
            pltpu.VMEM((8, TILE), F32),
            pltpu.VMEM((owners - 1, 8, TILE), F32),
            pltpu.SemaphoreType.DMA((4, 2 * nb)),
            pltpu.SemaphoreType.DMA((4, 2 * nb)),
            pltpu.SemaphoreType.DMA((owners - 1,)),
            pltpu.SemaphoreType.DMA((owners - 1,)),
        ],
        compiler_params=pltpu.CompilerParams(
            collective_id=0, has_side_effects=True, vmem_limit_bytes=48 * 1024 * 1024
        ),
    )(block_layer, gradients[0, 0])
    return out[None]


def solution(mesh):
    return jax.shard_map(
        functools.partial(per_device, mesh.shape["dp"], mesh.shape["owner"]),
        mesh=mesh,
        in_specs=(P("dp", "owner", None, None), P("owner")),
        out_specs=P("owner", "dp", None),
        check_vma=False,
    )
```

```python
import functools

import jax
import jax.numpy as jnp
from jax import lax
from jax.experimental import pallas as pl
from jax.experimental.pallas import tpu as pltpu
from jax.sharding import PartitionSpec as P

LAYERS = 4
ITERS = 3
TILE = 128
LAG = 1
BF16 = jnp.bfloat16
F32 = jnp.float32
MESH = pl.DeviceIdType.MESH


def mm(a, b):
    return jnp.dot(a.astype(BF16), b.astype(BF16), preferred_element_type=F32)


def upper_tiles(size_b):
    t = size_b // TILE
    return [(i, j) for i in range(t) for j in range(i, t)]


def pack(gram, acc_ref, first, size_b):
    tiles = upper_tiles(size_b)
    per_piece = acc_ref.shape[1] // TILE
    for n, (i, j) in enumerate(tiles):
        block = gram[i * TILE:(i + 1) * TILE, j * TILE:(j + 1) * TILE]
        row = n % per_piece * TILE
        acc_ref[first + n // per_piece, row:row + TILE, :] = block.astype(BF16)
    for n in range(len(tiles), 2 * per_piece):
        row = n % per_piece * TILE
        acc_ref[first + n // per_piece, row:row + TILE, :] = jnp.zeros((TILE, TILE), BF16)


def unpack(gath_ref, first, stat_ref, size_b):
    per_piece = gath_ref.shape[1] // TILE
    for n, (i, j) in enumerate(upper_tiles(size_b)):
        row = n % per_piece * TILE
        block = gath_ref[first + n // per_piece, row:row + TILE, :].astype(F32)
        stat_ref[i * TILE:(i + 1) * TILE, j * TILE:(j + 1) * TILE] = block
        if i != j:
            stat_ref[j * TILE:(j + 1) * TILE, i * TILE:(i + 1) * TILE] = block.T


def inverse_root(gath_ref, first, stat_ref, root_ref, size_b):
    unpack(gath_ref, first, stat_ref, size_b)
    rows = lax.broadcasted_iota(jnp.int32, (size_b, size_b), 0)
    cols = lax.broadcasted_iota(jnp.int32, (size_b, size_b), 1)
    diag = rows == cols
    stat = stat_ref[...]
    trace = jnp.sum(jnp.where(diag, stat, 0.0), keepdims=True)
    ridge = 0.01 * trace / size_b + 1e-06
    shifted = stat + jnp.where(diag, ridge, 0.0)
    norm2 = jnp.sum(shifted * shifted, keepdims=True)
    m = shifted * lax.rsqrt(norm2)
    a, y = 1.25, -0.25 * m
    for step in range(1, ITERS):
        yield
        square = mm(m, m)
        once = (25.0 * m - 10.0 * square + mm(m, square)) * 0.0625
        yield
        m = 1.5625 * once + mm((square - 10.0 * m) * 0.0625, once)
        y = 1.25 * y - (0.25 * a) * m - 0.25 * mm(y, m)
        a = 1.25 * a
    scale = lax.rsqrt(jnp.sqrt(jnp.sqrt(norm2)))
    root_ref[...] = (scale * (y + jnp.where(diag, a, 0.0))).astype(BF16)


def label_bit(me, number):
    d = 1 << number
    mine = me // d % 2
    return mine, me + d * (1 - 2 * mine)


class Piece:
    def __init__(self, index, me, order, acc, gath, landing, send, recv, target):
        self.index, self.me, self.order = index, me, order
        self.acc, self.gath, self.landing = acc, gath, landing
        self.send, self.recv, self.target = send, recv, target
        self.start_row, self.length = 0, acc.shape[0]
        self.copy, self.offset = None, 0

    def bit(self, number):
        return label_bit(self.me, number)

    def rows(self, first, length):
        return pl.ds(pl.multiple_of(first, 16), length)

    def start(self, step):
        last = len(self.order) - 1
        mine, partner = self.bit(self.order[last - abs(last - step)])
        if step < last:
            half = self.length // 2
            src = self.acc.at[self.rows(self.start_row + (1 - mine) * half, half)]
            dst = self.landing.at[pl.ds(self.offset, half)]
        elif step == last:
            src = self.acc.at[self.rows(self.start_row, self.length)]
            dst = self.landing.at[pl.ds(self.offset, self.length)]
        else:
            here = self.rows(self.start_row, self.length)
            src, dst = self.gath.at[here], self.gath.at[here]
        self.copy = pltpu.make_async_remote_copy(
            src_ref=src,
            dst_ref=dst,
            send_sem=self.send.at[self.index, step],
            recv_sem=self.recv.at[self.index, step],
            device_id=self.target(partner),
            device_id_type=MESH,
        )
        self.copy.start()

    def finish(self, step):
        last = len(self.order) - 1
        mine, _ = self.bit(self.order[last - abs(last - step)])
        self.copy.wait()
        if step <= last:
            if step < last:
                self.length //= 2
                self.start_row = self.start_row + mine * self.length
            keep = self.rows(self.start_row, self.length)
            arrived = self.landing[pl.ds(self.offset, self.length), :].astype(F32)
            total = (self.acc[keep, :].astype(F32) + arrived).astype(BF16)
            (self.acc if step < last else self.gath)[keep, :] = total
            self.offset += self.length
        else:
            self.start_row = self.start_row - mine * self.length
            self.length *= 2


def kernel(dp_count, owners, layer_ref, g_ref, out_ref, acc_s, gath_s, land_s, acc_g, gath_g,
           land_g, stats, roots, middle, middle_rows, e_src, e_buf, send, recv, e_send, e_recv):
    me = lax.axis_index("dp")
    own = lax.axis_index("owner")
    size_b = g_ref.shape[0]
    nb = dp_count.bit_length() - 1

    barrier = pltpu.get_barrier_semaphore()
    for number in range(nb):
        _, partner = label_bit(me, number)
        pl.semaphore_signal(barrier, inc=1, device_id=(partner, own), device_id_type=MESH)
    for j in range(1, owners):
        pl.semaphore_signal(
            barrier, inc=1, device_id=(me, lax.rem(own + j, owners)), device_id_type=MESH
        )

    order_a = list(range(nb))
    order_b = order_a[1::-1] + order_a[2:]
    target = lambda partner: (partner, own)
    orders = (order_a, order_b)
    left_pieces, right_pieces = (
        [
            Piece(n, me, orders[n % 2], acc_s.at[n], gath_s.at[n], land_s.at[n], send, recv, target)
            for n in pair
        ]
        for pair in ((0, 1), (2, 3))
    )
    grad_pieces = [
        Piece(4 + n, me, orders[n], acc_g.at[n], gath_g.at[n], land_g.at[n], send, recv, target)
        for n in range(2)
    ]
    g = g_ref[...]
    width = size_b // 2
    left = lax.dot_general(g, g, (((1,), (1,)), ((), ())), preferred_element_type=F32)
    pack(left, acc_s, 0, size_b)
    pl.semaphore_wait(barrier, nb + owners - 1)
    for piece in left_pieces:
        piece.start(0)
    right = lax.dot_general(g, g, (((0,), (0,)), ((), ())), preferred_element_type=F32)
    pack(right, acc_s, 2, size_b)
    for piece in right_pieces:
        piece.start(0)
    for n, piece in enumerate(grad_pieces):
        acc_g[n] = g[:, n * width:(n + 1) * width]
        piece.start(0)

    steps = 2 * nb - 1
    left_solve = inverse_root(gath_s, 0, stats.at[0], roots.at[0], size_b)
    right_solve = inverse_root(gath_s, 2, stats.at[1], roots.at[1], size_b)

    def attend(pieces, step):
        for piece in pieces:
            piece.finish(step)
            if step + 1 < steps:
                piece.start(step + 1)

    solvers = []

    def advance():
        while solvers:
            try:
                next(solvers[0])
                return
            except StopIteration:
                solvers.pop(0)

    for turn in range(steps + LAG):
        if turn < steps:
            attend(left_pieces, turn)
            if turn + 1 == steps:
                solvers.append(left_solve)
                advance()
            attend(right_pieces, turn)
            if turn + 1 == steps:
                solvers.append(right_solve)
                advance()
        if 0 <= turn - LAG < steps:
            attend(grad_pieces, turn - LAG)
            advance()
    while solvers:
        advance()

    height = out_ref.shape[0]
    mine_rows = pl.ds(pl.multiple_of(me * height, 16), height)
    halves = [slice(n * width, (n + 1) * width) for n in range(2)]
    right_root = roots[1]
    for n in range(2):
        middle[:, halves[n]] = jnp.dot(
            roots[0], gath_g[n], preferred_element_type=F32
        ).astype(BF16)
        middle_rows[:, halves[n]] = jnp.dot(
            roots[0, mine_rows, :], gath_g[n], preferred_element_type=F32
        )
    whole = jnp.dot(middle[...], right_root, preferred_element_type=F32) / dp_count
    energy = jnp.sum(whole * whole, keepdims=True)

    layer = layer_ref[0]
    sub = lax.broadcasted_iota(jnp.int32, e_src.shape, 0)
    lane = lax.broadcasted_iota(jnp.int32, e_src.shape, 1)
    mine = lane == layer
    value = jnp.where(sub == 0, energy, float(size_b * size_b))
    e_src[...] = jnp.where(mine, value, 0.0)
    copies = []
    for j in range(1, owners):
        copy = pltpu.make_async_remote_copy(
            src_ref=e_src,
            dst_ref=e_buf.at[j - 1],
            send_sem=e_send.at[j - 1],
            recv_sem=e_recv.at[j - 1],
            device_id=(me, lax.rem(own + j, owners)),
            device_id_type=MESH,
        )
        copy.start()
        copies.append(copy)
    high = middle_rows[...].astype(BF16)
    low = (middle_rows[...] - high.astype(F32)).astype(BF16)
    rows = jnp.dot(high, right_root, preferred_element_type=F32)
    rows = (rows + jnp.dot(low, right_root, preferred_element_type=F32)) / dp_count
    totals = e_src[...]
    for j, copy in enumerate(copies):
        copy.wait()
        totals += e_buf[j]
    energies = jnp.sum(jnp.where(mine & (sub == 0), totals, 0.0), keepdims=True)
    counts = jnp.sum(jnp.where(mine & (sub == 1), totals, 0.0), keepdims=True)
    out_ref[...] = (rows * lax.rsqrt(energies / counts + 1e-06)).astype(BF16)


def per_device(dp_count, owners, gradients, block_layer):
    size_b = gradients.shape[-1]
    nb = dp_count.bit_length() - 1
    used = len(upper_tiles(size_b)) * TILE
    unit = max(32 * dp_count, 2 * TILE)
    packed = -(-used // unit) * unit
    height = size_b // dp_count
    width = size_b // 2
    out = pl.pallas_call(
        functools.partial(kernel, dp_count, owners),
        out_shape=jax.ShapeDtypeStruct((height, size_b), BF16),
        in_specs=[
            pl.BlockSpec(memory_space=pltpu.SMEM),
            pl.BlockSpec(memory_space=pltpu.VMEM),
        ],
        out_specs=pl.BlockSpec(memory_space=pltpu.VMEM),
        scratch_shapes=[
            pltpu.VMEM((4, packed // 2, TILE), BF16),
            pltpu.VMEM((4, packed // 2, TILE), BF16),
            pltpu.VMEM((4, packed // 2, TILE), BF16),
            pltpu.VMEM((2, size_b, width), BF16),
            pltpu.VMEM((2, size_b, width), BF16),
            pltpu.VMEM((2, size_b, width), BF16),
            pltpu.VMEM((2, size_b, size_b), F32),
            pltpu.VMEM((2, size_b, size_b), BF16),
            pltpu.VMEM((size_b, size_b), BF16),
            pltpu.VMEM((height, size_b), F32),
            pltpu.VMEM((8, TILE), F32),
            pltpu.VMEM((owners - 1, 8, TILE), F32),
            pltpu.SemaphoreType.DMA((6, 2 * nb - 1)),
            pltpu.SemaphoreType.DMA((6, 2 * nb - 1)),
            pltpu.SemaphoreType.DMA((owners - 1,)),
            pltpu.SemaphoreType.DMA((owners - 1,)),
        ],
        compiler_params=pltpu.CompilerParams(
            collective_id=0, has_side_effects=True, vmem_limit_bytes=48 * 1024 * 1024
        ),
    )(block_layer, gradients[0, 0])
    return out[None]


def solution(mesh):
    return jax.shard_map(
        functools.partial(per_device, mesh.shape["dp"], mesh.shape["owner"]),
        mesh=mesh,
        in_specs=(P("dp", "owner", None, None), P("owner")),
        out_specs=P("owner", "dp", None),
        check_vma=False,
    )
```

```python
import functools

import jax
import jax.numpy as jnp
from jax import lax
from jax.experimental import pallas as pl
from jax.experimental.pallas import tpu as pltpu
from jax.sharding import PartitionSpec as P

LAYERS = 4
ITERS = 3
TILE = 128
LAG = 1
BF16 = jnp.bfloat16
F32 = jnp.float32
MESH = pl.DeviceIdType.MESH


def mm(a, b):
    return jnp.dot(a.astype(BF16), b.astype(BF16), preferred_element_type=F32)


def upper_tiles(size_b):
    t = size_b // TILE
    return [(i, j) for i in range(t) for j in range(i, t)]


def pack(gram, acc_ref, first, size_b):
    tiles = upper_tiles(size_b)
    per_piece = acc_ref.shape[1] // TILE
    for n, (i, j) in enumerate(tiles):
        block = gram[i * TILE:(i + 1) * TILE, j * TILE:(j + 1) * TILE]
        row = n % per_piece * TILE
        acc_ref[first + n // per_piece, row:row + TILE, :] = block.astype(BF16)
    for n in range(len(tiles), 2 * per_piece):
        row = n % per_piece * TILE
        acc_ref[first + n // per_piece, row:row + TILE, :] = jnp.zeros((TILE, TILE), BF16)


def unpack(gath_ref, first, stat_ref, size_b):
    per_piece = gath_ref.shape[1] // TILE
    for n, (i, j) in enumerate(upper_tiles(size_b)):
        row = n % per_piece * TILE
        block = gath_ref[first + n // per_piece, row:row + TILE, :].astype(F32)
        stat_ref[i * TILE:(i + 1) * TILE, j * TILE:(j + 1) * TILE] = block
        if i != j:
            stat_ref[j * TILE:(j + 1) * TILE, i * TILE:(i + 1) * TILE] = block.T


def inverse_root(gath_ref, first, stat_ref, root_ref, size_b):
    unpack(gath_ref, first, stat_ref, size_b)
    rows = lax.broadcasted_iota(jnp.int32, (size_b, size_b), 0)
    cols = lax.broadcasted_iota(jnp.int32, (size_b, size_b), 1)
    diag = rows == cols
    stat = stat_ref[...]
    trace = jnp.sum(jnp.where(diag, stat, 0.0), keepdims=True)
    ridge = 0.01 * trace / size_b + 1e-06
    shifted = stat + jnp.where(diag, ridge, 0.0)
    norm2 = jnp.sum(shifted * shifted, keepdims=True)
    m = shifted * lax.rsqrt(norm2)
    a, y = 1.25, -0.25 * m
    for step in range(1, ITERS):
        yield
        square = mm(m, m)
        once = (25.0 * m - 10.0 * square + mm(m, square)) * 0.0625
        yield
        m = 1.5625 * once + mm((square - 10.0 * m) * 0.0625, once)
        y = 1.25 * y - (0.25 * a) * m - 0.25 * mm(y, m)
        a = 1.25 * a
    scale = lax.rsqrt(jnp.sqrt(jnp.sqrt(norm2)))
    root_ref[...] = (scale * (y + jnp.where(diag, a, 0.0))).astype(BF16)


def label_bit(me, number):
    d = 1 << number
    mine = me // d % 2
    return mine, me + d * (1 - 2 * mine)


class Piece:
    def __init__(self, index, me, order, acc, gath, landing, send, recv, target):
        self.index, self.me, self.order = index, me, order
        self.acc, self.gath, self.landing = acc, gath, landing
        self.send, self.recv, self.target = send, recv, target
        self.start_row, self.length = 0, acc.shape[0]
        self.copy, self.offset = None, 0

    def bit(self, number):
        return label_bit(self.me, number)

    def rows(self, first, length):
        return pl.ds(pl.multiple_of(first, 16), length)

    def start(self, step):
        last = len(self.order) - 1
        mine, partner = self.bit(self.order[last - abs(last - step)])
        if step < last:
            half = self.length // 2
            src = self.acc.at[self.rows(self.start_row + (1 - mine) * half, half)]
            dst = self.landing.at[pl.ds(self.offset, half)]
        elif step == last:
            src = self.acc.at[self.rows(self.start_row, self.length)]
            dst = self.landing.at[pl.ds(self.offset, self.length)]
        else:
            here = self.rows(self.start_row, self.length)
            src, dst = self.gath.at[here], self.gath.at[here]
        self.copy = pltpu.make_async_remote_copy(
            src_ref=src,
            dst_ref=dst,
            send_sem=self.send.at[self.index, step],
            recv_sem=self.recv.at[self.index, step],
            device_id=self.target(partner),
            device_id_type=MESH,
        )
        self.copy.start()

    def finish(self, step):
        last = len(self.order) - 1
        mine, _ = self.bit(self.order[last - abs(last - step)])
        self.copy.wait()
        if step <= last:
            if step < last:
                self.length //= 2
                self.start_row = self.start_row + mine * self.length
            keep = self.rows(self.start_row, self.length)
            arrived = self.landing[pl.ds(self.offset, self.length), :].astype(F32)
            total = (self.acc[keep, :].astype(F32) + arrived).astype(BF16)
            (self.acc if step < last else self.gath)[keep, :] = total
            self.offset += self.length
        else:
            self.start_row = self.start_row - mine * self.length
            self.length *= 2


def kernel(dp_count, owners, layer_ref, g_ref, out_ref, acc_s, gath_s, land_s, acc_g, gath_g,
           land_g, stats, roots, middle, middle_rows, e_src, e_buf, send, recv, e_send, e_recv):
    me = lax.axis_index("dp")
    own = lax.axis_index("owner")
    size_b = g_ref.shape[0]
    nb = dp_count.bit_length() - 1

    barrier = pltpu.get_barrier_semaphore()
    for number in range(nb):
        _, partner = label_bit(me, number)
        pl.semaphore_signal(barrier, inc=1, device_id=(partner, own), device_id_type=MESH)
    for j in range(1, owners):
        pl.semaphore_signal(
            barrier, inc=1, device_id=(me, lax.rem(own + j, owners)), device_id_type=MESH
        )

    order_a = list(range(nb))
    order_b = order_a[1::-1] + order_a[2:]
    target = lambda partner: (partner, own)
    orders = (order_a, order_b)
    left_pieces, right_pieces = (
        [
            Piece(n, me, orders[n % 2], acc_s.at[n], gath_s.at[n], land_s.at[n], send, recv, target)
            for n in pair
        ]
        for pair in ((0, 1), (2, 3))
    )
    grad_pieces = [
        Piece(4 + n, me, orders[n], acc_g.at[n], gath_g.at[n], land_g.at[n], send, recv, target)
        for n in range(2)
    ]
    g = g_ref[...]
    width = size_b // 2
    left = lax.dot_general(g, g, (((1,), (1,)), ((), ())), preferred_element_type=F32)
    pack(left, acc_s, 0, size_b)
    pl.semaphore_wait(barrier, nb + owners - 1)
    for piece in left_pieces:
        piece.start(0)
    right = lax.dot_general(g, g, (((0,), (0,)), ((), ())), preferred_element_type=F32)
    pack(right, acc_s, 2, size_b)
    for piece in right_pieces:
        piece.start(0)
    for n in range(2):
        acc_g[n] = g[:, n * width:(n + 1) * width]

    steps = 2 * nb - 1
    left_solve = inverse_root(gath_s, 0, stats.at[0], roots.at[0], size_b)
    right_solve = inverse_root(gath_s, 2, stats.at[1], roots.at[1], size_b)

    def attend(pieces, step):
        for piece in pieces:
            piece.finish(step)
            if step + 1 < steps:
                piece.start(step + 1)

    solvers = []

    def advance():
        while solvers:
            try:
                next(solvers[0])
                return
            except StopIteration:
                solvers.pop(0)

    for turn in range(steps + LAG):
        if turn < steps:
            attend(left_pieces, turn)
            if turn + 1 == steps:
                solvers.append(left_solve)
                advance()
            attend(right_pieces, turn)
            if turn + 1 == steps:
                solvers.append(right_solve)
                advance()
        if turn == 0:
            for piece in grad_pieces:
                piece.start(0)
        if 0 <= turn - LAG < steps:
            attend(grad_pieces, turn - LAG)
            advance()
    while solvers:
        advance()

    height = out_ref.shape[0]
    mine_rows = pl.ds(pl.multiple_of(me * height, 16), height)
    halves = [slice(n * width, (n + 1) * width) for n in range(2)]
    right_root = roots[1]
    for n in range(2):
        middle[:, halves[n]] = jnp.dot(
            roots[0], gath_g[n], preferred_element_type=F32
        ).astype(BF16)
        middle_rows[:, halves[n]] = jnp.dot(
            roots[0, mine_rows, :], gath_g[n], preferred_element_type=F32
        )
    whole = jnp.dot(middle[...], right_root, preferred_element_type=F32) / dp_count
    energy = jnp.sum(whole * whole, keepdims=True)

    layer = layer_ref[0]
    sub = lax.broadcasted_iota(jnp.int32, e_src.shape, 0)
    lane = lax.broadcasted_iota(jnp.int32, e_src.shape, 1)
    mine = lane == layer
    value = jnp.where(sub == 0, energy, float(size_b * size_b))
    e_src[...] = jnp.where(mine, value, 0.0)
    copies = []
    for j in range(1, owners):
        copy = pltpu.make_async_remote_copy(
            src_ref=e_src,
            dst_ref=e_buf.at[j - 1],
            send_sem=e_send.at[j - 1],
            recv_sem=e_recv.at[j - 1],
            device_id=(me, lax.rem(own + j, owners)),
            device_id_type=MESH,
        )
        copy.start()
        copies.append(copy)
    high = middle_rows[...].astype(BF16)
    low = (middle_rows[...] - high.astype(F32)).astype(BF16)
    rows = jnp.dot(high, right_root, preferred_element_type=F32)
    rows = (rows + jnp.dot(low, right_root, preferred_element_type=F32)) / dp_count
    totals = e_src[...]
    for j, copy in enumerate(copies):
        copy.wait()
        totals += e_buf[j]
    energies = jnp.sum(jnp.where(mine & (sub == 0), totals, 0.0), keepdims=True)
    counts = jnp.sum(jnp.where(mine & (sub == 1), totals, 0.0), keepdims=True)
    out_ref[...] = (rows * lax.rsqrt(energies / counts + 1e-06)).astype(BF16)


def per_device(dp_count, owners, gradients, block_layer):
    size_b = gradients.shape[-1]
    nb = dp_count.bit_length() - 1
    used = len(upper_tiles(size_b)) * TILE
    unit = max(32 * dp_count, 2 * TILE)
    packed = -(-used // unit) * unit
    height = size_b // dp_count
    width = size_b // 2
    out = pl.pallas_call(
        functools.partial(kernel, dp_count, owners),
        out_shape=jax.ShapeDtypeStruct((height, size_b), BF16),
        in_specs=[
            pl.BlockSpec(memory_space=pltpu.SMEM),
            pl.BlockSpec(memory_space=pltpu.VMEM),
        ],
        out_specs=pl.BlockSpec(memory_space=pltpu.VMEM),
        scratch_shapes=[
            pltpu.VMEM((4, packed // 2, TILE), BF16),
            pltpu.VMEM((4, packed // 2, TILE), BF16),
            pltpu.VMEM((4, packed // 2, TILE), BF16),
            pltpu.VMEM((2, size_b, width), BF16),
            pltpu.VMEM((2, size_b, width), BF16),
            pltpu.VMEM((2, size_b, width), BF16),
            pltpu.VMEM((2, size_b, size_b), F32),
            pltpu.VMEM((2, size_b, size_b), BF16),
            pltpu.VMEM((size_b, size_b), BF16),
            pltpu.VMEM((height, size_b), F32),
            pltpu.VMEM((8, TILE), F32),
            pltpu.VMEM((owners - 1, 8, TILE), F32),
            pltpu.SemaphoreType.DMA((6, 2 * nb - 1)),
            pltpu.SemaphoreType.DMA((6, 2 * nb - 1)),
            pltpu.SemaphoreType.DMA((owners - 1,)),
            pltpu.SemaphoreType.DMA((owners - 1,)),
        ],
        compiler_params=pltpu.CompilerParams(
            collective_id=0, has_side_effects=True, vmem_limit_bytes=48 * 1024 * 1024
        ),
    )(block_layer, gradients[0, 0])
    return out[None]


def solution(mesh):
    return jax.shard_map(
        functools.partial(per_device, mesh.shape["dp"], mesh.shape["owner"]),
        mesh=mesh,
        in_specs=(P("dp", "owner", None, None), P("owner")),
        out_specs=P("owner", "dp", None),
        check_vma=False,
    )
```
